32 devices in a mesh: rows: 8 (over y, x, core), rep: 4 (over z).
Axes of the slice: x: 2, y: 2, z: 4, core: 2. Of those that a mesh axis runs over, the one named last changes fastest.
Arguments:
- x_tiles: bfloat16 [64, 10, 128, 128], P('rows'), may hold values from -2.5 to 2.5
- giant_tiles: bfloat16 [64, 10, 128, 128], P('rows'), may hold values from -2.5 to 2.5
- coeffs: float32 [3], replicated, may hold values from 0.5 to 1.5
- pattern: int32 [64, 10], replicated, may hold values from 0 to 63, as said below
Outputs:
- squared: bfloat16 [64, 10, 128, 128], P('rows')
- result: bfloat16 [64, 10, 128, 128], P('rows')
The draws below stay inside these ranges and needn't reach their ends.
Inputs may be any that keep to these rules, and one draw needn't show every extreme that they name: `pattern`: slots 2 j and 2 j + 1 of block row i hold two different tile columns of panel (i // 8 + j - 2) mod (8), a panel being 8 consecutive block rows, for j = 0 to 4; slot 4 holds i itself.
All inputs are finite; a program needn't handle non-finite values.
Results may differ from the reference program's by a relative error of at most 0.012.
Values may be sent and summed in bfloat16 or wider, within the bound.
No kernel may reach another device: no remote copies, remote signals or barrier semaphores. Data moves between devices by JAX's collectives and lax.ppermute only.
A program may use at most 128 MiB of HBM per device.

```python
import jax
import jax.numpy as jnp
from jax import lax

TILE = 128
RB = 8
HALF = 2
KP = 2
K = 10
NB = 64


def draw_pattern(key, part):
    panel_count = NB // RB
    block_rows = jnp.arange(NB, dtype=jnp.int32)
    home = block_rows // RB
    within = block_rows % RB
    spread = 2 * HALF + 1
    first_key, second_key = jax.random.split(jax.random.fold_in(key, 17))
    first = jax.random.randint(first_key, (NB, spread), 0, RB, dtype=jnp.int32)
    first = jnp.where(jnp.arange(spread, dtype=jnp.int32)[None, :] == HALF, within[:, None], first)
    second = (first + jax.random.randint(second_key, (NB, spread), 1, RB, dtype=jnp.int32)) % RB
    panel = (home[:, None] + jnp.arange(spread, dtype=jnp.int32)[None, :] - HALF) % panel_count
    both = jnp.stack([panel * RB + first, panel * RB + second], axis=-1)
    return both.reshape(NB, spread * 2).astype(jnp.int32)


def block_scale(key, dims, cuts, smallest, top_value):
    gain, own = 1.0, jax.random.fold_in(key, 6)
    for position, shards_of in cuts:
        steps = jnp.exp(jax.random.uniform(jax.random.fold_in(own, position), (shards_of,), jnp.float32, smallest / len(cuts), top_value / len(cuts)))
        gain = gain * jnp.repeat(steps, dims[position] // shards_of).reshape([-1 if axis == position else 1 for axis in range(len(dims))])
    return gain


def gaussian(key, dims, deviation, most, cuts=(), kind=jnp.bfloat16):
    drawn = jax.random.normal(key, dims, jnp.float32) * deviation
    if len(cuts) > 0:
        drawn = block_scale(key, dims, cuts, -0.22, 0.18) * drawn
    return jnp.clip(drawn, min=-most, max=most).astype(kind)


def setup_inputs(seed: int = 0) -> dict:
    key_list = jax.random.split(jax.random.key(seed), 5)
    return {
        "x_tiles": gaussian(key_list[0], (NB, K, TILE, TILE), (2.0 / TILE ** 0.5), 2.5, ((0, 8),)),
        "giant_tiles": gaussian(key_list[1], (NB, K, TILE, TILE), (2.0 / TILE ** 0.5), 2.5, ((0, 8),)),
        "coeffs": jnp.clip(jax.random.uniform(key_list[2], (3,), jnp.float32, 0.5, 1.5), 0.5, 1.5),
        "pattern": draw_pattern(jax.random.fold_in(key_list[4], 71), 0),
    }


def truncated(left, right, pattern):
    def one_row(index):
        columns = pattern[index]
        left_row = left[index].astype(jnp.float32)
        right_rows = right[columns].astype(jnp.float32)
        right_cols = pattern[columns]
        matches = (right_cols[:, :, None] == columns[None, None, :]).astype(jnp.float32)
        chosen = jnp.einsum('stu,stxy->suxy', matches, right_rows, precision=lax.Precision.HIGHEST)
        return jnp.einsum('sxz,suzy->uxy', left_row, chosen, precision=lax.Precision.HIGHEST)

    return lax.map(one_row, jnp.arange(NB, dtype=jnp.int32))


def reference(x_tiles, giant_tiles, coeffs, pattern):
    squared = truncated(x_tiles, x_tiles, pattern).astype(jnp.bfloat16)
    diagonal_slot = (jnp.arange(K, dtype=jnp.int32) == HALF * KP).astype(jnp.float32)
    identity = diagonal_slot[:, None, None] * jnp.eye(TILE, dtype=jnp.float32)[None, :, :]
    baby = coeffs[0] * identity[None] + coeffs[1] * x_tiles.astype(jnp.float32) + coeffs[2] * squared.astype(jnp.float32)
    baby = baby.astype(jnp.bfloat16)
    result = truncated(giant_tiles, baby, pattern).astype(jnp.bfloat16)
    return squared, result
```

```python
import functools

import jax
import jax.numpy as jnp
from jax import lax
from jax.experimental import pallas as pl
from jax.experimental.pallas import tpu as pltpu
from jax.sharding import PartitionSpec as P

HALF = 2
KP = 2
CLASSES = 2 * HALF


def down_offset(panel, kind):
    return (kind - panel + HALF) % CLASSES - HALF


def up_offset(panel, kind):
    return (kind - panel + HALF - 1) % CLASSES - HALF + 1


def classes_of(rep):
    return (rep % 2, rep % 2 + 2)


def route(panels, reps, target, kept=lambda panel, rep: True):
    pairs = []
    for rep in range(reps):
        for panel in range(panels):
            to_panel, to_rep = target(panel, rep)
            to_panel %= panels
            if kept(to_panel, to_rep):
                pairs.append((panel * reps + rep, to_panel * reps + to_rep))
    return pairs


def permute(block, pairs):
    return lax.ppermute(block, ("rows", "rep"), pairs)


def tile_table(pattern, device, blocks):
    count = pattern.shape[1]
    unit = blocks * KP
    even = device % 2 == 0
    mine = lax.dynamic_slice_in_dim(pattern, device * blocks, blocks, 0)
    rows = jnp.take(pattern, mine, axis=0, mode="clip")
    same = rows[:, :, :, None] == mine[:, None, None, :]
    slots = jnp.arange(count, dtype=jnp.int32)
    found = jnp.max(jnp.where(same, slots[None, None, :, None], -1), axis=2)
    offset = slots // KP - HALF
    turned = jnp.where(even, offset, -offset)
    far = jnp.where(turned == 1, 2, jnp.where(turned == -1, 3, jnp.where(turned == -HALF, 4, 5)))
    own = jnp.where((offset == HALF) == even, 0, 1)
    region = jnp.where(offset[:, None] == 0, own[None, :], far[:, None])
    place = region[None] * unit + (mine % blocks)[:, :, None] * KP + found % KP
    return jnp.where(found >= 0, place, 6 * unit).reshape(-1)


def product_kernel(first, facts, table, coeffs, left, own0, own1, core, near, two, forwarded, *rest):
    if first:
        full, main, extra, send0, send1, right, sums, baby, in_sems, out_sems = rest
    else:
        full, main, extra, right, sums, in_sems, out_sems = rest
    blocks, count, tile = left.shape[0], left.shape[1], left.shape[2]
    unit = blocks * KP
    sources = (own0, own1, core, near, two, forwarded)
    loads = [
        pltpu.make_async_copy(source, right.at[pl.ds(k * unit, unit)], in_sems.at[k])
        for k, source in enumerate(sources)
    ]
    for load in loads:
        load.start()
    right[6 * unit] = jnp.zeros((tile, tile), right.dtype)
    offset = facts[0]
    even = facts[1]
    for load in loads:
        load.wait()

    def one_unit(which, slot):
        def one_row(i, carry):
            lefts = jnp.concatenate([left[i, s] for s in range(count)], axis=1)
            rights = jnp.concatenate(
                [
                    jnp.concatenate(
                        [right[table[(i * count + s) * count + slot + e]] for e in range(KP)], axis=1
                    )
                    for s in range(count)
                ],
                axis=0,
            )
            total = jnp.dot(lefts, rights, preferred_element_type=jnp.float32)
            rounded = total.astype(jnp.bfloat16)
            for e in range(KP):
                part = rounded[:, e * tile : (e + 1) * tile]
                sums[which, i, e] = part
                if first:
                    mixed = coeffs[1] * left[i, slot + e].astype(jnp.float32) + coeffs[
                        2
                    ] * part.astype(jnp.float32)
                    if e == 0:
                        on = jnp.where(slot == HALF * KP, coeffs[0], 0.0)
                        line = lax.broadcasted_iota(jnp.int32, (tile, tile), 0)
                        column = lax.broadcasted_iota(jnp.int32, (tile, tile), 1)
                        mixed = jnp.where(line == column, on, 0.0) + mixed
                    baby[which, i, e] = mixed.astype(jnp.bfloat16)
            return carry

        lax.fori_loop(0, blocks, one_row, 0)

    def put(source, target, k):
        return pltpu.make_async_copy(source, target, out_sems.at[k])

    low = pl.multiple_of((offset + HALF) * KP, KP)
    high = 2 * HALF * KP
    both = offset == -HALF
    one_unit(0, low)
    stores = [put(sums.at[0], full.at[:, pl.ds(low, KP)], 0), put(sums.at[0], main, 1)]
    for store in stores:
        store.start()

    @pl.when(both)
    def _():
        one_unit(1, high)
        put(sums.at[1], full.at[:, pl.ds(high, KP)], 2).start()
        put(sums.at[1], extra, 3).start()

    more = []
    if first:
        upper = jnp.where(both, 1, 0)
        more.append(put(baby.at[jnp.where(even == 1, upper, 0)], send0, 4))
        more.append(put(baby.at[jnp.where(even == 1, 0, upper)], send1, 5))
    for store in more:
        store.start()
    for store in stores + more:
        store.wait()

    @pl.when(both)
    def _():
        put(sums.at[1], full.at[:, pl.ds(high, KP)], 2).wait()
        put(sums.at[1], extra, 3).wait()


def product(first, facts, table, coeffs, left, rights, full):
    blocks, count, tile = left.shape[0], left.shape[1], left.shape[2]
    unit = blocks * KP
    unit_shape = jax.ShapeDtypeStruct((blocks, KP, tile, tile), left.dtype)
    whole = jax.ShapeDtypeStruct(left.shape, left.dtype)
    smem = pl.BlockSpec(memory_space=pltpu.SMEM)
    hbm = pl.BlockSpec(memory_space=pl.ANY)
    vmem = pl.BlockSpec(memory_space=pltpu.VMEM)
    flat = [r.reshape(unit, tile, tile) for r in rights]
    outs = [whole] + [unit_shape] * (4 if first else 2)
    pair = pltpu.VMEM((2, blocks, KP, tile, tile), left.dtype)
    operands = [facts, table, coeffs, left] + flat
    specs = [smem] * 3 + [vmem] + [hbm] * 6
    kernel = functools.partial(product_kernel, first)
    aliases = {}
    if full is not None:
        operands.append(full)
        specs.append(hbm)
        aliases = {len(operands) - 1: 0}
        inner = kernel

        def kernel(*refs):
            inner(*refs[:10], *refs[11:])

    return pl.pallas_call(
        kernel,
        out_shape=outs,
        in_specs=specs,
        out_specs=[hbm] * len(outs),
        scratch_shapes=[pltpu.VMEM((6 * unit + 1, tile, tile), left.dtype), pair]
        + ([pair] if first else [])
        + [pltpu.SemaphoreType.DMA((6,)), pltpu.SemaphoreType.DMA((6,))],
        input_output_aliases=aliases,
        name="product_first" if first else "product_second",
        cost_estimate=pl.CostEstimate(
            flops=2 * blocks * count * KP * tile**3, bytes_accessed=2 * 2**20 * 4, transcendentals=0
        ),
    )(*operands)


def place_kernel(facts, full_in, main, extra, full, sems):
    del full_in
    offset = facts[0]
    low = pl.multiple_of((offset + HALF) * KP, KP)
    high = 2 * HALF * KP
    store = pltpu.make_async_copy(main, full.at[:, pl.ds(low, KP)], sems.at[0])
    more = pltpu.make_async_copy(extra, full.at[:, pl.ds(high, KP)], sems.at[1])
    store.start()

    @pl.when(offset == -HALF)
    def _():
        more.start()
        more.wait()

    store.wait()


def place(facts, full, main, extra):
    hbm = pl.BlockSpec(memory_space=pl.ANY)
    vmem = pl.BlockSpec(memory_space=pltpu.VMEM)
    return pl.pallas_call(
        place_kernel,
        out_shape=jax.ShapeDtypeStruct(full.shape, full.dtype),
        in_specs=[pl.BlockSpec(memory_space=pltpu.SMEM), hbm, vmem, vmem],
        out_specs=hbm,
        scratch_shapes=[pltpu.SemaphoreType.DMA((2,))],
        input_output_aliases={1: 0},
        name="place",
        cost_estimate=pl.CostEstimate(flops=2**24, bytes_accessed=2**21, transcendentals=0),
    )(facts, full, main, extra)


def local(x_tiles, giant_tiles, coeffs, pattern):
    blocks = x_tiles.shape[0]
    panels = lax.axis_size("rows")
    reps = lax.axis_size("rep")
    device = lax.axis_index("rows")
    rep = lax.axis_index("rep")
    even = device % 2 == 0

    def swapped(panel):
        return panel + 1 if panel % 2 == 0 else panel - 1

    core_route = route(panels, reps, lambda p, z: (swapped(p), z))
    near_route = route(panels, reps, lambda p, z: (p - 1 if p % 2 == 0 else p + 1, z))

    def two_route(chunk):
        return route(
            panels,
            reps,
            lambda p, z: (p + 2 if p % 2 == 0 else p - 2, z),
            lambda p, z: (classes_of(z)[chunk] - p) % CLASSES != (1 if p % 2 == 0 else 3),
        )

    partner_route = route(panels, reps, lambda p, z: (p, z ^ 1))

    def extra_route(chunk):
        return route(
            panels,
            reps,
            lambda p, z: (p, z ^ 1),
            lambda p, z: down_offset(p, classes_of(z ^ 1)[chunk]) == -HALF,
        )

    def gathered(chunk, send0, send1):
        near = permute(send1, near_route)
        two = permute(send0, two_route(chunk))
        core = permute(send0, core_route)
        forwarded = permute(near, core_route)
        return (send0, send1, core, near, two, forwarded)

    def facts_of(kind):
        return jnp.stack([down_offset(device, kind), even.astype(jnp.int32)]).astype(jnp.int32)

    kinds = classes_of(rep)
    others = classes_of(1 - rep % 2)
    rights = []
    for chunk in range(2):
        up = (up_offset(device, kinds[chunk]) + HALF) * KP
        down = (down_offset(device, kinds[chunk]) + HALF) * KP
        send0 = lax.dynamic_slice_in_dim(x_tiles, jnp.where(even, up, down), KP, 1)
        send1 = lax.dynamic_slice_in_dim(x_tiles, jnp.where(even, down, up), KP, 1)
        rights.append(gathered(chunk, send0, send1))
    table = tile_table(pattern, device, blocks)

    squared = None
    result = None
    babies = []
    for chunk in range(2):
        squared, main, extra, send0, send1 = product(
            True, facts_of(kinds[chunk]), table, coeffs, x_tiles, rights[chunk], squared
        )
        babies.append(gathered(chunk, send0, send1))
        main = permute(main, partner_route)
        extra = permute(extra, extra_route(chunk))
        squared = place(facts_of(others[chunk]), squared, main, extra)
    for chunk in range(2):
        result, main, extra = product(
            False, facts_of(kinds[chunk]), table, coeffs, giant_tiles, babies[chunk], result
        )
        main = permute(main, partner_route)
        extra = permute(extra, extra_route(chunk))
        result = place(facts_of(others[chunk]), result, main, extra)
    return (squared, result)


def solution(mesh):
    return jax.shard_map(
        local,
        mesh=mesh,
        in_specs=(P("rows", None, None, None), P("rows", None, None, None), P(), P()),
        out_specs=(P("rows", None, None, None), P("rows", None, None, None)),
        check_vma=False,
    )
```

```python
import functools

import jax
import jax.numpy as jnp
from jax import lax
from jax.experimental import pallas as pl
from jax.experimental.pallas import tpu as pltpu
from jax.sharding import PartitionSpec as P


HALF = 2
KP = 2
CLASSES = 2 * HALF

COST = 2**20
VMEM_LIMIT = 16 * 2**20


def down_offset(panel, kind):
    return (kind - panel + HALF) % CLASSES - HALF


def up_offset(panel, kind):
    return (kind - panel + HALF - 1) % CLASSES - HALF + 1


def classes_of(rep):
    return (rep % 2, rep % 2 + 2)


def route(panels, reps, target, kept=lambda panel, rep: True):
    pairs = []
    for rep in range(reps):
        for panel in range(panels):
            to_panel, to_rep = target(panel, rep)
            to_panel %= panels
            if kept(to_panel, to_rep):
                pairs.append((panel * reps + rep, to_panel * reps + to_rep))
    return pairs


def permute(block, pairs):
    return lax.ppermute(block, ("rows", "rep"), pairs)


def tile_table(pattern, device, blocks):
    count = pattern.shape[1]
    unit = blocks * KP
    even = device % 2 == 0
    mine = lax.dynamic_slice_in_dim(pattern, device * blocks, blocks, 0)
    rows = jnp.take(pattern, mine, axis=0, mode="clip")
    same = rows[:, :, :, None] == mine[:, None, None, :]
    slots = jnp.arange(count, dtype=jnp.int32)
    found = jnp.max(jnp.where(same, slots[None, None, :, None], -1), axis=2)
    offset = slots // KP - HALF
    turned = jnp.where(even, offset, -offset)
    far = jnp.where(turned == 1, 2, jnp.where(turned == -1, 3, jnp.where(turned == -HALF, 4, 5)))
    own = jnp.where((offset == HALF) == even, 0, 1)
    region = jnp.where(offset[:, None] == 0, own[None, :], far[:, None])
    place = region[None] * unit + (mine % blocks)[:, :, None] * KP + found % KP
    return jnp.where(found >= 0, place, 6 * unit).reshape(-1)


def product_kernel(first, aliased, facts, table, coeffs, left_hbm, *refs):
    sources, refs = refs[:6], refs[6 + aliased :]
    if first:
        full, main, extra, send0, send1, left, right, sums, baby, left_sems, in_sems, out_sem = refs
    else:
        full, main, extra, left, right, sums, left_sems, in_sems, out_sem = refs
    blocks, count, tile = left.shape[0], left.shape[1], left.shape[2]
    unit = blocks * KP
    loads = [
        pltpu.make_async_copy(source, right.at[pl.ds(k * unit, unit)], in_sems.at[k])
        for k, source in enumerate(sources)
    ]

    def left_load(i):
        return pltpu.make_async_copy(left_hbm.at[i], left.at[i], left_sems.at[i])

    for load in loads:
        load.start()
    for i in range(blocks):
        left_load(i).start()
    right[6 * unit] = jnp.zeros((tile, tile), right.dtype)
    offset = facts[0]
    even = facts[1]
    both = offset == -HALF
    for load in loads:
        load.wait()

    def out_copies(which, slot, i):
        copies = [(sums.at[which, i], full.at[i, pl.ds(slot, KP)])]
        if which == 0:
            copies.append((sums.at[0, i], main.at[i]))
        else:
            copies.append((sums.at[1, i], extra.at[i]))
        return [pltpu.make_async_copy(a, b, out_sem) for a, b in copies]

    def one_unit(which, slot, begin, end):
        def one_row(i, carry):
            if which == 0:
                left_load(i).wait()
            lefts = jnp.concatenate([left[i, s] for s in range(begin, end)], axis=1)
            rights = jnp.concatenate(
                [
                    jnp.concatenate(
                        [right[table[(i * count + s) * count + slot + e]] for e in range(KP)], axis=1
                    )
                    for s in range(begin, end)
                ],
                axis=0,
            )
            total = jnp.dot(lefts, rights, preferred_element_type=jnp.float32)
            rounded = total.astype(jnp.bfloat16)
            for e in range(KP):
                part = rounded[:, e * tile : (e + 1) * tile]
                sums[which, i, e] = part
                if first:
                    mixed = coeffs[1] * left[i, slot + e].astype(jnp.float32) + coeffs[
                        2
                    ] * part.astype(jnp.float32)
                    if e == 0:
                        on = jnp.where(slot == HALF * KP, coeffs[0], 0.0)
                        line = lax.broadcasted_iota(jnp.int32, (tile, tile), 0)
                        column = lax.broadcasted_iota(jnp.int32, (tile, tile), 1)
                        mixed = jnp.where(line == column, on, 0.0) + mixed
                    baby[which, i, e] = mixed.astype(jnp.bfloat16)
            for copy in out_copies(which, slot, i):
                copy.start()
            return carry

        lax.fori_loop(0, blocks, one_row, 0)

    low = pl.multiple_of((offset + HALF) * KP, KP)
    high = 2 * HALF * KP
    for o in range(-HALF, HALF):

        @pl.when(offset == o)
        def _(o=o):
            begin = max(0, o) * KP
            end = (2 * HALF + 1 + min(0, o)) * KP
            one_unit(0, (o + HALF) * KP, begin, end)
            if o == -HALF:
                one_unit(1, high, HALF * KP, count)

    tail = []
    if first:
        upper = jnp.where(both, 1, 0)
        tail = [
            pltpu.make_async_copy(baby.at[jnp.where(even == 1, upper, 0)], send0, in_sems.at[0]),
            pltpu.make_async_copy(baby.at[jnp.where(even == 1, 0, upper)], send1, in_sems.at[1]),
        ]
    for copy in tail:
        copy.start()
    for copy in tail:
        copy.wait()
    for i in range(blocks):
        for copy in out_copies(0, low, i):
            copy.wait()

    @pl.when(both)
    def _():
        for i in range(blocks):
            for copy in out_copies(1, high, i):
                copy.wait()


def product(first, facts, table, coeffs, left, rights, full):
    blocks, tile = left.shape[0], left.shape[2]
    unit = blocks * KP
    unit_shape = jax.ShapeDtypeStruct((blocks, KP, tile, tile), left.dtype)
    whole = jax.ShapeDtypeStruct(left.shape, left.dtype)
    smem = pl.BlockSpec(memory_space=pltpu.SMEM)
    hbm = pl.BlockSpec(memory_space=pl.ANY)
    flat = [r.reshape(unit, tile, tile) for r in rights]
    outs = [whole] + [unit_shape] * (4 if first else 2)
    pair = pltpu.VMEM((2, blocks, KP, tile, tile), left.dtype)
    operands = [facts, table, coeffs, left] + flat
    if full is not None:
        operands.append(full)
    return pl.pallas_call(
        functools.partial(product_kernel, first, full is not None),
        out_shape=outs,
        in_specs=[smem] * 3 + [hbm] * (len(operands) - 3),
        out_specs=[pl.BlockSpec(memory_space=pltpu.HBM)] * len(outs),
        scratch_shapes=[
            pltpu.VMEM(left.shape, left.dtype),
            pltpu.VMEM((6 * unit + 1, tile, tile), left.dtype),
            pair,
        ]
        + ([pair] if first else [])
        + [
            pltpu.SemaphoreType.DMA((blocks,)),
            pltpu.SemaphoreType.DMA((6,)),
            pltpu.SemaphoreType.DMA,
        ],
        input_output_aliases={} if full is None else {len(operands) - 1: 0},
        compiler_params=pltpu.CompilerParams(vmem_limit_bytes=VMEM_LIMIT),
        name="product_first" if first else "product_second",
        cost_estimate=pl.CostEstimate(flops=COST, bytes_accessed=2**23, transcendentals=0),
    )(*operands)


def place_kernel(facts, full_in, main, extra, full, held, sems):
    del full_in
    offset = facts[0]
    low = pl.multiple_of((offset + HALF) * KP, KP)
    high = 2 * HALF * KP
    blocks = held.shape[1]
    half = blocks // 2
    both = offset == -HALF

    def rows(k):
        return pl.ds(k * half, half)

    def load(which, k):
        source = main if which == 0 else extra
        return pltpu.make_async_copy(source.at[rows(k)], held.at[which, rows(k)], sems.at[which, k])

    def store(which, k):
        slot = low if which == 0 else high
        return pltpu.make_async_copy(
            held.at[which, rows(k)], full.at[rows(k), pl.ds(slot, KP)], sems.at[which, k]
        )

    def run(units):
        steps = [(which, k) for which in units for k in range(2)]
        for step in steps:
            load(*step).start()
        for step in steps:
            load(*step).wait()
            store(*step).start()
        for step in steps:
            store(*step).wait()

    @pl.when(both)
    def _():
        run((0, 1))

    @pl.when(jnp.logical_not(both))
    def _():
        run((0,))


def place(facts, full, main, extra):
    hbm = pl.BlockSpec(memory_space=pl.ANY)
    return pl.pallas_call(
        place_kernel,
        out_shape=jax.ShapeDtypeStruct(full.shape, full.dtype),
        in_specs=[pl.BlockSpec(memory_space=pltpu.SMEM), hbm, hbm, hbm],
        out_specs=hbm,
        scratch_shapes=[
            pltpu.VMEM((2,) + main.shape, main.dtype),
            pltpu.SemaphoreType.DMA((2, 2)),
        ],
        input_output_aliases={1: 0},
        compiler_params=pltpu.CompilerParams(vmem_limit_bytes=VMEM_LIMIT),
        name="place",
        cost_estimate=pl.CostEstimate(flops=COST, bytes_accessed=2**21, transcendentals=0),
    )(facts, full, main, extra)


def local(x_tiles, giant_tiles, coeffs, pattern):
    blocks = x_tiles.shape[0]
    panels = lax.axis_size("rows")
    reps = lax.axis_size("rep")
    device = lax.axis_index("rows")
    rep = lax.axis_index("rep")
    even = device % 2 == 0

    def swapped(panel):
        return panel + 1 if panel % 2 == 0 else panel - 1

    core_route = route(panels, reps, lambda p, z: (swapped(p), z))
    near_route = route(panels, reps, lambda p, z: (p - 1 if p % 2 == 0 else p + 1, z))

    def two_route(chunk):
        return route(
            panels,
            reps,
            lambda p, z: (p + 2 if p % 2 == 0 else p - 2, z),
            lambda p, z: (classes_of(z)[chunk] - p) % CLASSES != (1 if p % 2 == 0 else 3),
        )

    partner_route = route(panels, reps, lambda p, z: (p, z ^ 1))

    def extra_route(chunk):
        return route(
            panels,
            reps,
            lambda p, z: (p, z ^ 1),
            lambda p, z: down_offset(p, classes_of(z ^ 1)[chunk]) == -HALF,
        )

    def gathered(chunk, send0, send1):
        near = permute(send1, near_route)
        two = permute(send0, two_route(chunk))
        core = permute(send0, core_route)
        forwarded = permute(near, core_route)
        return (send0, send1, core, near, two, forwarded)

    def swapped_parts(chunk, main, extra):
        main = permute(main, partner_route)
        extra = permute(extra, extra_route(chunk))
        return main, extra

    def facts_of(kind):
        return jnp.stack([down_offset(device, kind), even.astype(jnp.int32)]).astype(jnp.int32)

    kinds = classes_of(rep)
    others = classes_of(1 - rep % 2)
    rights = []
    for chunk in range(2):
        up = (up_offset(device, kinds[chunk]) + HALF) * KP
        down = (down_offset(device, kinds[chunk]) + HALF) * KP
        send0 = lax.dynamic_slice_in_dim(x_tiles, jnp.where(even, up, down), KP, 1)
        send1 = lax.dynamic_slice_in_dim(x_tiles, jnp.where(even, down, up), KP, 1)
        rights.append(gathered(chunk, send0, send1))
    table = tile_table(pattern, device, blocks)

    squared = None
    result = None
    babies = []
    arrived = []
    for chunk in range(2):
        squared, main, extra, send0, send1 = product(
            True, facts_of(kinds[chunk]), table, coeffs, x_tiles, rights[chunk], squared
        )
        babies.append(gathered(chunk, send0, send1))
        arrived.append(swapped_parts(chunk, main, extra))
    for chunk in range(2):
        squared = place(facts_of(others[chunk]), squared, *arrived[chunk])
    arrived = []
    for chunk in range(2):
        result, main, extra = product(
            False, facts_of(kinds[chunk]), table, coeffs, giant_tiles, babies[chunk], result
        )
        arrived.append(swapped_parts(chunk, main, extra))
    for chunk in range(2):
        result = place(facts_of(others[chunk]), result, *arrived[chunk])
    return (squared, result)


def solution(mesh):
    return jax.shard_map(
        local,
        mesh=mesh,
        in_specs=(P("rows", None, None, None), P("rows", None, None, None), P(), P()),
        out_specs=(P("rows", None, None, None), P("rows", None, None, None)),
        check_vma=False,
    )
```

```python
import functools

import jax
import jax.numpy as jnp
from jax import lax
from jax.experimental import pallas as pl
from jax.experimental.pallas import tpu as pltpu
from jax.sharding import PartitionSpec as P


HALF = 2
KP = 2
CLASSES = 2 * HALF

COST = 2**20
VMEM_LIMIT = 16 * 2**20


def down_offset(panel, kind):
    return (kind - panel + HALF) % CLASSES - HALF


def up_offset(panel, kind):
    return (kind - panel + HALF - 1) % CLASSES - HALF + 1


def classes_of(rep):
    return (rep % 2, rep % 2 + 2)


def route(panels, reps, target, kept=lambda panel, rep: True):
    pairs = []
    for rep in range(reps):
        for panel in range(panels):
            to_panel, to_rep = target(panel, rep)
            to_panel %= panels
            if kept(to_panel, to_rep):
                pairs.append((panel * reps + rep, to_panel * reps + to_rep))
    return pairs


def permute(block, pairs):
    return lax.ppermute(block, ("rows", "rep"), pairs)


def tile_table(pattern, device, blocks):
    count = pattern.shape[1]
    unit = blocks * KP
    even = device % 2 == 0
    mine = lax.dynamic_slice_in_dim(pattern, device * blocks, blocks, 0)
    rows = jnp.take(pattern, mine, axis=0, mode="clip")
    same = rows[:, :, :, None] == mine[:, None, None, :]
    slots = jnp.arange(count, dtype=jnp.int32)
    found = jnp.max(jnp.where(same, slots[None, None, :, None], -1), axis=2)
    offset = slots // KP - HALF
    turned = jnp.where(even, offset, -offset)
    far = jnp.where(turned == 1, 2, jnp.where(turned == -1, 3, jnp.where(turned == -HALF, 4, 5)))
    own = jnp.where((offset == HALF) == even, 0, 1)
    region = jnp.where(offset[:, None] == 0, own[None, :], far[:, None])
    place = region[None] * unit + (mine % blocks)[:, :, None] * KP + found % KP
    return jnp.where(found >= 0, place, 6 * unit).reshape(-1)


def row_product(left, right, table, i, slot, begin, end):
    count = left.shape[1]
    lefts = jnp.concatenate([left[i, s] for s in range(begin, end)], axis=1)
    rights = jnp.concatenate(
        [
            jnp.concatenate(
                [right[table[(i * count + s) * count + slot + e]] for e in range(KP)], axis=1
            )
            for s in range(begin, end)
        ],
        axis=0,
    )
    return jnp.dot(lefts, rights, preferred_element_type=jnp.float32)


def low_slot(offset):
    return pl.multiple_of((offset + HALF) * KP, KP)


def first_kernel(aliased, facts, table, coeffs, left_hbm, *refs):
    sources, refs = refs[:6], refs[6 + aliased :]
    full, main, extra, send0, send1, left, right, sums, baby, left_sems, in_sems, out_sem = refs
    blocks, count, tile = left.shape[0], left.shape[1], left.shape[2]
    unit = blocks * KP
    high = 2 * HALF * KP
    loads = [
        pltpu.make_async_copy(source, right.at[pl.ds(k * unit, unit)], in_sems.at[k])
        for k, source in enumerate(sources)
    ]

    def left_load(i):
        return pltpu.make_async_copy(left_hbm.at[i], left.at[i], left_sems.at[i])

    for load in loads:
        load.start()
    for i in range(blocks):
        left_load(i).start()
    right[6 * unit] = jnp.zeros((tile, tile), right.dtype)
    offset = facts[0]
    even = facts[1] == 1
    both = offset == -HALF
    for load in loads:
        load.wait()

    def put(source, target):
        return pltpu.make_async_copy(source, target, out_sem)

    def one_unit(which, slot, begin, end):
        def one_row(i, carry):
            if which == 0:
                left_load(i).wait()
            total = row_product(left, right, table, i, slot, begin, end)
            rounded = total.astype(jnp.bfloat16)
            for e in range(KP):
                part = rounded[:, e * tile : (e + 1) * tile]
                sums[which, i, e] = part
                mixed = coeffs[1] * left[i, slot + e].astype(jnp.float32) + coeffs[2] * part.astype(
                    jnp.float32
                )
                if slot + e == HALF * KP:
                    line = lax.broadcasted_iota(jnp.int32, (tile, tile), 0)
                    column = lax.broadcasted_iota(jnp.int32, (tile, tile), 1)
                    mixed = jnp.where(line == column, coeffs[0], 0.0) + mixed
                baby[which, i, e] = mixed.astype(jnp.bfloat16)
            put(sums.at[which, i], full.at[i, pl.ds(slot, KP)]).start()
            put(sums.at[which, i], (extra if which else main).at[i]).start()
            if begin == 0 and slot == 0 or which:
                @pl.when(even if which else jnp.logical_not(even))
                def _():
                    put(baby.at[which, i], send0.at[i]).start()

                @pl.when(jnp.logical_not(even) if which else even)
                def _():
                    put(baby.at[which, i], send1.at[i]).start()
            else:
                put(baby.at[which, i], send0.at[i]).start()
                put(baby.at[which, i], send1.at[i]).start()
            return carry

        lax.fori_loop(0, blocks, one_row, 0)

    for o in range(-HALF, HALF):

        @pl.when(offset == o)
        def _(o=o):
            begin = max(0, o) * KP
            end = (2 * HALF + 1 + min(0, o)) * KP
            one_unit(0, (o + HALF) * KP, begin, end)
            if o == -HALF:
                one_unit(1, high, HALF * KP, count)

    put(sums.at[0], main).wait()
    put(sums.at[0], full.at[:, pl.ds(low_slot(offset), KP)]).wait()
    put(baby.at[0], send0).wait()
    put(baby.at[0], send1).wait()

    @pl.when(both)
    def _():
        put(sums.at[1], extra).wait()
        put(sums.at[1], full.at[:, pl.ds(high, KP)]).wait()


SMEM_SPEC = pl.BlockSpec(memory_space=pltpu.SMEM)
ANY_SPEC = pl.BlockSpec(memory_space=pl.ANY)
HBM_SPEC = pl.BlockSpec(memory_space=pltpu.HBM)


def call(kernel, operands, scalars, outs, scratch, full_at=None, space=ANY_SPEC):
    return pl.pallas_call(
        kernel,
        out_shape=outs,
        in_specs=[SMEM_SPEC] * scalars + [space] * (len(operands) - scalars),
        out_specs=[HBM_SPEC] * len(outs),
        scratch_shapes=scratch,
        input_output_aliases={} if full_at is None else {full_at: 0},
        compiler_params=pltpu.CompilerParams(vmem_limit_bytes=VMEM_LIMIT),
        cost_estimate=pl.CostEstimate(flops=COST, bytes_accessed=2**23, transcendentals=0),
    )(*operands)


def units_of(blocks, tile, dtype):
    return jax.ShapeDtypeStruct((blocks, KP, tile, tile), dtype)


def first_product(facts, table, coeffs, left, rights, full):
    blocks, tile = left.shape[0], left.shape[2]
    unit = blocks * KP
    flat = [r.reshape(unit, tile, tile) for r in rights]
    operands = [facts, table, coeffs, left] + flat + ([] if full is None else [full])
    pair = pltpu.VMEM((2, blocks, KP, tile, tile), left.dtype)
    return call(
        functools.partial(first_kernel, full is not None),
        operands,
        3,
        [jax.ShapeDtypeStruct(left.shape, left.dtype)] + [units_of(blocks, tile, left.dtype)] * 4,
        [
            pltpu.VMEM(left.shape, left.dtype),
            pltpu.VMEM((6 * unit + 1, tile, tile), left.dtype),
            pair,
            pair,
            pltpu.SemaphoreType.DMA((blocks,)),
            pltpu.SemaphoreType.DMA((6,)),
            pltpu.SemaphoreType.DMA,
        ],
        None if full is None else len(operands) - 1,
    )


EARLY_REGIONS = (0, 1, 2, 3, 5)


def early_kernel(aliased, facts, table, left_hbm, *refs):
    sources, refs = refs[:5], refs[5 + aliased :]
    full, extra, partial, left, right, sums, totals, left_sems, in_sems, out_sem = refs
    blocks, count, tile = left.shape[0], left.shape[1], left.shape[2]
    unit = blocks * KP
    high = 2 * HALF * KP
    loads = [
        pltpu.make_async_copy(source, right.at[pl.ds(k * unit, unit)], in_sems.at[k])
        for k, source in zip(EARLY_REGIONS, sources)
    ]

    def left_load(i):
        return pltpu.make_async_copy(left_hbm.at[i], left.at[i], left_sems.at[i])

    for load in loads:
        load.start()
    for i in range(blocks):
        left_load(i).start()
    right[6 * unit] = jnp.zeros((tile, tile), right.dtype)
    offset = facts[0]
    even = facts[1] == 1
    both = offset == -HALF
    for load in loads:
        load.wait()

    def put(source, target):
        return pltpu.make_async_copy(source, target, out_sem)

    def whole_unit(slot, begin, end):
        def one_row(i, carry):
            left_load(i).wait()
            total = row_product(left, right, table, i, slot, begin, end)
            rounded = total.astype(jnp.bfloat16)
            for e in range(KP):
                sums[i, e] = rounded[:, e * tile : (e + 1) * tile]
            put(sums.at[i], full.at[i, pl.ds(slot, KP)]).start()
            put(sums.at[i], extra.at[i]).start()
            return carry

        lax.fori_loop(0, blocks, one_row, 0)

    def part_unit(loaded, slot, begin, end):
        def one_row(i, carry):
            if not loaded:
                left_load(i).wait()
            totals[i] = row_product(left, right, table, i, slot, begin, end)
            put(totals.at[i], partial.at[i]).start()
            return carry

        lax.fori_loop(0, blocks, one_row, 0)

    for parity in range(2):
        first, last = (KP, count) if parity == 0 else (0, count - KP)
        for o in range(-HALF, HALF):

            @pl.when(jnp.logical_and(offset == o, even if parity == 0 else jnp.logical_not(even)))
            def _(o=o, parity=parity, first=first, last=last):
                if o > -HALF:
                    begin = max(0, o) * KP
                    end = (2 * HALF + 1 + min(0, o)) * KP
                    part_unit(False, (o + HALF) * KP, max(begin, first), min(end, last))
                elif parity == 0:
                    whole_unit(high, HALF * KP, count)
                    part_unit(True, 0, first, (HALF + 1) * KP)
                else:
                    whole_unit(0, 0, (HALF + 1) * KP)
                    part_unit(True, high, HALF * KP, last)

    put(totals, partial).wait()

    @pl.when(both)
    def _():
        put(sums, extra).wait()
        put(sums, full.at[:, pl.ds(0, KP)]).wait()


def early_product(facts, table, left, rights, full):
    blocks, tile = left.shape[0], left.shape[2]
    unit = blocks * KP
    flat = [rights[k].reshape(unit, tile, tile) for k in EARLY_REGIONS]
    operands = [facts, table, left] + flat + ([] if full is None else [full])
    return call(
        functools.partial(early_kernel, full is not None),
        operands,
        2,
        [
            jax.ShapeDtypeStruct(left.shape, left.dtype),
            units_of(blocks, tile, left.dtype),
            jax.ShapeDtypeStruct((blocks, tile, KP * tile), jnp.float32),
        ],
        [
            pltpu.VMEM(left.shape, left.dtype),
            pltpu.VMEM((6 * unit + 1, tile, tile), left.dtype),
            pltpu.VMEM((blocks, KP, tile, tile), left.dtype),
            pltpu.VMEM((blocks, tile, KP * tile), jnp.float32),
            pltpu.SemaphoreType.DMA((blocks,)),
            pltpu.SemaphoreType.DMA((6,)),
            pltpu.SemaphoreType.DMA,
        ],
        None if full is None else len(operands) - 1,
    )


def late_kernel(facts, table, left_hbm, two, partial, full_in, full, main, *refs):
    del full_in
    left, right, sums, totals, in_sems, total_sems, out_sem = refs
    blocks, tile = left.shape[0], left.shape[2]
    count = left_hbm.shape[1]
    unit = blocks * KP
    offset = facts[0]
    even = facts[1] == 1
    both = offset == -HALF
    begin = jnp.where(even, 0, count - KP)
    slot = jnp.where(jnp.logical_and(both, jnp.logical_not(even)), 2 * HALF * KP, (offset + HALF) * KP)
    loads = [
        pltpu.make_async_copy(two, right.at[pl.ds(0, unit)], in_sems.at[0]),
        pltpu.make_async_copy(left_hbm.at[:, pl.ds(begin, KP)], left, in_sems.at[1]),
    ]

    def total_load(i):
        return pltpu.make_async_copy(partial.at[i], totals.at[i], total_sems.at[i])

    def put(source, target):
        return pltpu.make_async_copy(source, target, out_sem)

    for load in loads:
        load.start()
    for i in range(blocks):
        total_load(i).start()
    right[unit] = jnp.zeros((tile, tile), right.dtype)
    for load in loads:
        load.wait()

    def one_row(i, carry):
        total_load(i).wait()
        lefts = jnp.concatenate([left[i, s] for s in range(KP)], axis=1)
        rights = jnp.concatenate(
            [
                jnp.concatenate(
                    [
                        right[jnp.minimum(table[(i * count + begin + s) * count + slot + e] - 4 * unit, unit)]
                        for e in range(KP)
                    ],
                    axis=1,
                )
                for s in range(KP)
            ],
            axis=0,
        )
        total = totals[i] + jnp.dot(lefts, rights, preferred_element_type=jnp.float32)
        rounded = total.astype(jnp.bfloat16)
        for e in range(KP):
            sums[i, e] = rounded[:, e * tile : (e + 1) * tile]
        put(sums.at[i], main.at[i]).start()
        put(sums.at[i], full.at[i, pl.ds(slot, KP)]).start()
        return carry

    lax.fori_loop(0, blocks, one_row, 0)
    put(sums, main).wait()
    put(sums, full.at[:, pl.ds(slot, KP)]).wait()


def late_product(facts, table, left, two, partial, full):
    blocks, tile = left.shape[0], left.shape[2]
    unit = blocks * KP
    return call(
        late_kernel,
        [facts, table, left, two.reshape(unit, tile, tile), partial, full],
        2,
        [jax.ShapeDtypeStruct(left.shape, left.dtype), units_of(blocks, tile, left.dtype)],
        [
            pltpu.VMEM((blocks, KP, tile, tile), left.dtype),
            pltpu.VMEM((unit + 1, tile, tile), left.dtype),
            pltpu.VMEM((blocks, KP, tile, tile), left.dtype),
            pltpu.VMEM((blocks, tile, KP * tile), jnp.float32),
            pltpu.SemaphoreType.DMA((2,)),
            pltpu.SemaphoreType.DMA((blocks,)),
            pltpu.SemaphoreType.DMA,
        ],
        5,
    )


PIECES = 4


def place_kernel(number, facts, full_in, *refs):
    del full_in
    parts, (full, held, load_sems, store_sems) = refs[:number], refs[number:]
    rows = held.shape[1] // PIECES

    def load(k, piece):
        where = pl.ds(piece * rows, rows)
        return pltpu.make_async_copy(parts[k].at[where], held.at[k, where], load_sems.at[k, piece])

    def store(k, piece):
        where = pl.ds(piece * rows, rows)
        target = full.at[where, pl.ds(facts[2 * k], KP)]
        return pltpu.make_async_copy(held.at[k, where], target, store_sems.at[k, piece])

    def each(step):
        for k in range(number):

            @pl.when(facts[2 * k + 1] == 1)
            def _(k=k):
                for piece in range(PIECES):
                    step(k, piece)

    def move(k, piece):
        load(k, piece).wait()
        store(k, piece).start()

    each(lambda k, piece: load(k, piece).start())
    each(move)
    each(lambda k, piece: store(k, piece).wait())


def place(full, parts):
    number = len(parts)
    facts = jnp.stack([jnp.asarray(f, jnp.int32) for slot, counts, _ in parts for f in (slot, counts)])
    units = [unit for _, _, unit in parts]
    return call(
        functools.partial(place_kernel, number),
        [facts, full] + units,
        1,
        [jax.ShapeDtypeStruct(full.shape, full.dtype)],
        [
            pltpu.VMEM((number,) + units[0].shape, full.dtype),
            pltpu.SemaphoreType.DMA((number, PIECES)),
            pltpu.SemaphoreType.DMA((number, PIECES)),
        ],
        1,
    )[0]


def pick_kernel(slots, tiles, out0, out1, held, load_sems, store_sems):
    outs = (out0, out1)
    loads = [
        pltpu.make_async_copy(tiles.at[:, pl.ds(slots[k], KP)], held.at[k], load_sems.at[k])
        for k in range(2)
    ]
    stores = [pltpu.make_async_copy(held.at[k], outs[k], store_sems.at[k]) for k in range(2)]
    for load in loads:
        load.start()
    for load, store in zip(loads, stores):
        load.wait()
        store.start()
    for store in stores:
        store.wait()


def pick(tiles, slot0, slot1):
    blocks, tile = tiles.shape[0], tiles.shape[2]
    return call(
        pick_kernel,
        [jnp.stack([slot0, slot1]).astype(jnp.int32), tiles],
        1,
        [units_of(blocks, tile, tiles.dtype)] * 2,
        [
            pltpu.VMEM((2, blocks, KP, tile, tile), tiles.dtype),
            pltpu.SemaphoreType.DMA((2,)),
            pltpu.SemaphoreType.DMA((2,)),
        ],
        space=HBM_SPEC,
    )


def local(x_tiles, giant_tiles, coeffs, pattern):
    blocks = x_tiles.shape[0]
    panels = lax.axis_size("rows")
    reps = lax.axis_size("rep")
    device = lax.axis_index("rows")
    rep = lax.axis_index("rep")
    even = device % 2 == 0

    def swapped(panel):
        return panel + 1 if panel % 2 == 0 else panel - 1

    core_route = route(panels, reps, lambda p, z: (swapped(p), z))
    near_route = route(panels, reps, lambda p, z: (p - 1 if p % 2 == 0 else p + 1, z))

    def two_route(chunk):
        return route(
            panels,
            reps,
            lambda p, z: (p + 2 if p % 2 == 0 else p - 2, z),
            lambda p, z: (classes_of(z)[chunk] - p) % CLASSES != (1 if p % 2 == 0 else 3),
        )

    partner_route = route(panels, reps, lambda p, z: (p, z ^ 1))

    def extra_route(chunk):
        return route(
            panels,
            reps,
            lambda p, z: (p, z ^ 1),
            lambda p, z: down_offset(p, classes_of(z ^ 1)[chunk]) == -HALF,
        )

    def gathered(chunk, send0, send1):
        near = permute(send1, near_route)
        two = permute(send0, two_route(chunk))
        core = permute(send0, core_route)
        forwarded = permute(near, core_route)
        return (send0, send1, core, near, two, forwarded)

    def swapped_parts(chunk, main, extra):
        main = permute(main, partner_route)
        extra = permute(extra, extra_route(chunk))
        return main, extra

    def facts_of(kind):
        return jnp.stack([down_offset(device, kind), even.astype(jnp.int32)]).astype(jnp.int32)

    kinds = classes_of(rep)
    others = classes_of(1 - rep % 2)
    rights = []
    for chunk in range(2):
        up = (up_offset(device, kinds[chunk]) + HALF) * KP
        down = (down_offset(device, kinds[chunk]) + HALF) * KP
        send0, send1 = pick(x_tiles, jnp.where(even, up, down), jnp.where(even, down, up))
        rights.append(gathered(chunk, send0, send1))
    table = tile_table(pattern, device, blocks)
    unit = blocks * KP
    early_table = jnp.where(table // unit == 4, 6 * unit, table)

    squared = None
    babies = []
    parts = []
    top = 2 * HALF * KP
    for chunk in range(2):
        squared, main, extra, send0, send1 = first_product(
            facts_of(kinds[chunk]), table, coeffs, x_tiles, rights[chunk], squared
        )
        babies.append(gathered(chunk, send0, send1))
        main, extra = swapped_parts(chunk, main, extra)
        low = (down_offset(device, others[chunk]) + HALF) * KP
        parts += [(low, 1, main), (top, low == 0, extra)]
    squared = place(squared, parts)

    result = None
    parts = []
    for chunk in range(2):
        facts = facts_of(kinds[chunk])
        result, extra, partial = early_product(
            facts, early_table, giant_tiles, babies[chunk], result
        )
        result, main = late_product(facts, table, giant_tiles, babies[chunk][4], partial, result)
        main, extra = swapped_parts(chunk, main, extra)
        low = (down_offset(device, others[chunk]) + HALF) * KP
        both = low == 0
        late = jnp.where(both & ~even, top, low)
        parts += [(jnp.where(even, top, 0), both, extra), (late, 1, main)]
    result = place(result, parts[:-1])
    result = place(result, parts[-1:])
    return (squared, result)


def solution(mesh):
    return jax.shard_map(
        local,
        mesh=mesh,
        in_specs=(P("rows", None, None, None), P("rows", None, None, None), P(), P()),
        out_specs=(P("rows", None, None, None), P("rows", None, None, None)),
        check_vma=False,
    )
```

```python
import functools

import jax
import jax.numpy as jnp
from jax import lax
from jax.experimental import pallas as pl
from jax.experimental.pallas import tpu as pltpu
from jax.sharding import PartitionSpec as P


HALF = 2
KP = 2
CLASSES = 2 * HALF

COST = 2**20
VMEM_LIMIT = 16 * 2**20


def down_offset(panel, kind):
    return (kind - panel + HALF) % CLASSES - HALF


def classes_of(rep):
    return (rep % 2, rep % 2 + 2)


def route(panels, reps, target, kept=lambda panel, rep: True):
    pairs = []
    for rep in range(reps):
        for panel in range(panels):
            to_panel, to_rep = target(panel, rep)
            to_panel %= panels
            if kept(to_panel, to_rep):
                pairs.append((panel * reps + rep, to_panel * reps + to_rep))
    return pairs


def permute(block, pairs):
    return lax.ppermute(block, ("rows", "rep"), pairs)


def table_kernel(pattern, table, *, blocks):
    count = pattern.shape[1]
    device = lax.axis_index("rows")

    def one_row(i, carry):
        mine = [pattern[device * blocks + i, u] for u in range(count)]
        for s in range(count):
            theirs = [pattern[mine[s], t] for t in range(count)]
            place = lax.rem(mine[s], blocks) * KP
            for u in range(count):
                offset = u // KP - s // KP
                found = jnp.int32(-1)
                if abs(offset) <= HALF:
                    for e in range(KP):
                        same = theirs[(offset + HALF) * KP + e] == mine[u]
                        found = jnp.where(same, place + e, found)
                table[(i * count + s) * count + u] = found
        return carry

    lax.fori_loop(0, blocks, one_row, 0)


def here(chunk, swapped=False):
    device, rep = lax.axis_index("rows"), lax.axis_index("rep")
    parity = lax.rem(rep + 1 if swapped else rep, 2)
    return down_offset(device, parity + 2 * chunk), lax.rem(device, 2) == 0


def row_product(left, regions, table, i, slot, begin, end):
    count = left.shape[1]

    def met(s, e):
        where = table[(i * count + s) * count + slot + e]
        tile = regions[s // KP][jnp.maximum(where, 0)]
        return jnp.where(where >= 0, tile, jnp.zeros_like(tile))

    lefts = jnp.concatenate([left[i, s] for s in range(begin, end)], axis=1)
    rights = jnp.concatenate(
        [jnp.concatenate([met(s, e) for e in range(KP)], axis=1) for s in range(begin, end)], axis=0
    )
    return jnp.dot(lefts, rights, preferred_element_type=jnp.float32)


def regions_of(parity, offset, own0, own1, core, near, two, forwarded):
    own = own0 if (offset == HALF) == (parity == 0) else own1
    if parity == 0:
        return (two, near, own, core, forwarded)
    return (forwarded, core, own, near, two)


def bounds_of(offset):
    return max(0, offset) * KP, (2 * HALF + 1 + min(0, offset)) * KP


def branches(chunk, run):
    mine, even = here(chunk)
    for parity in range(2):
        for offset in range(-HALF, HALF):

            @pl.when(jnp.logical_and(mine == offset, even == (parity == 0)))
            def _(parity=parity, offset=offset):
                run(parity, offset)


def halves(total):
    rounded = total.astype(jnp.bfloat16)
    tile = total.shape[0]
    return [rounded[:, e * tile : (e + 1) * tile] for e in range(KP)]


def first_kernel(chunk, table, coeffs, left, *refs):
    sources, (main, extra, send0, send1) = refs[:6], refs[6:]
    blocks, tile = left.shape[0], left.shape[2]

    def one_unit(parity, offset, sums, sends):
        slot = (offset + HALF) * KP
        regions = regions_of(parity, offset, *sources)

        def one_row(i, carry):
            total = row_product(left, regions, table, i, slot, *bounds_of(offset))
            for e, part in enumerate(halves(total)):
                sums[i, e] = part
                mixed = coeffs[1] * left[i, slot + e].astype(jnp.float32) + coeffs[2] * part.astype(
                    jnp.float32
                )
                if slot + e == HALF * KP:
                    line = lax.broadcasted_iota(jnp.int32, (tile, tile), 0)
                    column = lax.broadcasted_iota(jnp.int32, (tile, tile), 1)
                    mixed = jnp.where(line == column, coeffs[0], 0.0) + mixed
                for send in sends:
                    send[i, e] = mixed.astype(jnp.bfloat16)
            return carry

        lax.fori_loop(0, blocks, one_row, 0)

    def run(parity, offset):
        if offset > -HALF:
            one_unit(parity, offset, main, (send0, send1))
        else:
            one_unit(parity, -HALF, main, (send1 if parity == 0 else send0,))
            one_unit(parity, HALF, extra, (send0 if parity == 0 else send1,))

    branches(chunk, run)


def early_kernel(chunk, table, left, own0, own1, core, near, forwarded, extra, partial):
    blocks, count = left.shape[0], left.shape[1]

    def regions(parity, offset):
        return regions_of(parity, offset, own0, own1, core, near, None, forwarded)

    def whole_unit(parity, offset):
        def one_row(i, carry):
            total = row_product(
                left, regions(parity, offset), table, i, (offset + HALF) * KP, *bounds_of(offset)
            )
            for e, part in enumerate(halves(total)):
                extra[i, e] = part
            return carry

        lax.fori_loop(0, blocks, one_row, 0)

    def part_unit(parity, offset):
        begin, end = bounds_of(offset)
        begin, end = (max(begin, KP), end) if parity == 0 else (begin, min(end, count - KP))

        def one_row(i, carry):
            partial[i] = row_product(
                left, regions(parity, offset), table, i, (offset + HALF) * KP, begin, end
            )
            return carry

        lax.fori_loop(0, blocks, one_row, 0)

    def run(parity, offset):
        if offset > -HALF:
            part_unit(parity, offset)
        else:
            sign = 1 if parity == 0 else -1
            whole_unit(parity, sign * HALF)
            part_unit(parity, -sign * HALF)

    branches(chunk, run)


def late_kernel(chunk, table, left, two, partial, main):
    blocks, count = left.shape[0], left.shape[1]
    offset, even = here(chunk)
    odd = jnp.logical_not(even)
    slot = jnp.where(jnp.logical_and(offset == -HALF, odd), 2 * HALF, offset + HALF) * KP

    def rows(begin):
        def one_row(i, carry):
            total = partial[i] + row_product(
                left, (two,) * count, table, i, slot, begin, begin + KP
            )
            for e, part in enumerate(halves(total)):
                main[i, e] = part
            return carry

        lax.fori_loop(0, blocks, one_row, 0)

    pl.when(odd)(lambda: rows(count - KP))
    pl.when(jnp.logical_not(odd))(lambda: rows(0))


def call(kernel, operands, outs, scratch=(), full_at=None):
    arrays, specs = [], []
    for space, array in operands:
        specs.append(pl.BlockSpec(memory_space=space))
        if space in (pltpu.VMEM, pltpu.HBM):
            array = pltpu.with_memory_space_constraint(array, space)
        arrays.append(array)
    return pl.pallas_call(
        kernel,
        out_shape=[space(out.shape, out.dtype) for space, out in outs],
        in_specs=specs,
        out_specs=[pl.BlockSpec(memory_space=space) for space, _ in outs],
        scratch_shapes=scratch,
        input_output_aliases={} if full_at is None else {full_at: 0},
        compiler_params=pltpu.CompilerParams(vmem_limit_bytes=VMEM_LIMIT),
        cost_estimate=pl.CostEstimate(flops=COST, bytes_accessed=2**23, transcendentals=0),
    )(*arrays)


def units_of(tiles):
    blocks, tile = tiles.shape[0], tiles.shape[2]
    return pltpu.VMEM, jax.ShapeDtypeStruct((blocks, KP, tile, tile), tiles.dtype)


def flat(block):
    return pltpu.VMEM, block.reshape((-1,) + block.shape[2:])


def first_product(chunk, table, coeffs, left, rights):
    operands = [(pltpu.SMEM, table), (pltpu.SMEM, coeffs), (pltpu.VMEM, left)]
    return call(
        functools.partial(first_kernel, chunk),
        operands + [flat(r) for r in rights],
        [units_of(left)] * 4,
    )


def early_product(chunk, table, left, rights):
    rights = rights[:4] + rights[5:]
    blocks, tile = left.shape[0], left.shape[2]
    partial = jax.ShapeDtypeStruct((blocks, tile, KP * tile), jnp.float32)
    return call(
        functools.partial(early_kernel, chunk),
        [(pltpu.SMEM, table), (pltpu.VMEM, left)] + [flat(r) for r in rights],
        [units_of(left), (pltpu.VMEM, partial)],
    )


def late_product(chunk, table, left, two, partial):
    return call(
        functools.partial(late_kernel, chunk),
        [(pltpu.SMEM, table), (pltpu.VMEM, left), flat(two), (pltpu.VMEM, partial)],
        [units_of(left)],
    )[0]


def place_kernel(names, aliased, *refs):
    parts, full, sems = refs[aliased : aliased + len(names)], refs[-2], refs[-1]
    slots, counts = [], []
    for chunk, swapped, second, mirrored in names:
        offset, even = here(chunk, swapped)
        both = offset == -HALF
        low = (offset + HALF) * KP
        high = 2 * HALF * KP
        turned = jnp.logical_and(both, jnp.logical_not(even))
        if second:
            slots.append(jnp.where(even, high, 0) if mirrored else high)
            counts.append(both)
        else:
            slots.append(jnp.where(turned, high, low) if mirrored else low)
            counts.append(None)

    def store(k):
        target = full.at[:, pl.ds(slots[k], KP)]
        return pltpu.make_async_copy(parts[k], target, sems.at[k])

    for step in (lambda k: store(k).start(), lambda k: store(k).wait()):
        for k, count in enumerate(counts):
            if count is None:
                step(k)
            else:
                pl.when(count)(functools.partial(step, k))


def place(shape, full, parts):
    names = tuple(name for name, _ in parts)
    units = [(pltpu.VMEM, unit) for _, unit in parts]
    aliased = 0 if full is None else 1
    return call(
        functools.partial(place_kernel, names, aliased),
        [(pltpu.HBM, full)] * aliased + units,
        [(pltpu.HBM, shape)],
        [pltpu.SemaphoreType.DMA((len(parts),))],
        0 if aliased else None,
    )[0]


def pick_kernel(chunk, tiles, out0, out1, sems):
    down, even = here(chunk)
    up = jnp.where(down == -HALF, HALF, down)
    offsets = (jnp.where(even, up, down), jnp.where(even, down, up))
    loads = [
        pltpu.make_async_copy(tiles.at[:, pl.ds((offsets[k] + HALF) * KP, KP)], out, sems.at[k])
        for k, out in enumerate((out0, out1))
    ]
    for load in loads:
        load.start()
    for load in loads:
        load.wait()


def pick(chunk, tiles):
    return call(
        functools.partial(pick_kernel, chunk),
        [(pltpu.HBM, tiles)],
        [units_of(tiles)] * 2,
        [pltpu.SemaphoreType.DMA((2,))],
    )


def tile_table(pattern, blocks):
    size = blocks * pattern.shape[1] ** 2
    return call(
        functools.partial(table_kernel, blocks=blocks),
        [(pltpu.SMEM, pattern)],
        [(pltpu.SMEM, jax.ShapeDtypeStruct((size,), jnp.int32))],
    )[0]


def local(x_tiles, giant_tiles, coeffs, pattern):
    blocks = x_tiles.shape[0]
    panels = lax.axis_size("rows")
    reps = lax.axis_size("rep")

    def swapped(panel):
        return panel + 1 if panel % 2 == 0 else panel - 1

    core_route = route(panels, reps, lambda p, z: (swapped(p), z))
    near_route = route(panels, reps, lambda p, z: (p - 1 if p % 2 == 0 else p + 1, z))

    def two_route(chunk):
        return route(
            panels,
            reps,
            lambda p, z: (p + 2 if p % 2 == 0 else p - 2, z),
            lambda p, z: (classes_of(z)[chunk] - p) % CLASSES != (1 if p % 2 == 0 else 3),
        )

    partner_route = route(panels, reps, lambda p, z: (p, z ^ 1))

    def extra_route(chunk):
        return route(
            panels,
            reps,
            lambda p, z: (p, z ^ 1),
            lambda p, z: down_offset(p, classes_of(z ^ 1)[chunk]) == -HALF,
        )

    def gathered(chunk, send0, send1):
        near = permute(send1, near_route)
        two = permute(send0, two_route(chunk))
        core = permute(send0, core_route)
        forwarded = permute(near, core_route)
        return (send0, send1, core, near, two, forwarded)

    def swapped_parts(chunk, main, extra):
        main = permute(main, partner_route)
        extra = permute(extra, extra_route(chunk))
        return main, extra

    rights = []
    for chunk in range(2):
        send0, send1 = pick(chunk, x_tiles)
        rights.append(gathered(chunk, send0, send1))
    table = tile_table(pattern, blocks)
    shape = jax.ShapeDtypeStruct(x_tiles.shape, x_tiles.dtype)

    babies = []
    parts = []
    for chunk in range(2):
        main, extra, send0, send1 = first_product(
            chunk, table, coeffs, x_tiles, rights[chunk]
        )
        babies.append(gathered(chunk, send0, send1))
        parts += [((chunk, False, False, False), main), ((chunk, False, True, False), extra)]
        main, extra = swapped_parts(chunk, main, extra)
        parts += [((chunk, True, False, False), main), ((chunk, True, True, False), extra)]
    squared = place(shape, None, parts)

    parts = []
    for chunk in range(2):
        extra, partial = early_product(chunk, table, giant_tiles, babies[chunk])
        main = late_product(chunk, table, giant_tiles, babies[chunk][4], partial)
        parts += [((chunk, False, True, True), extra), ((chunk, False, False, True), main)]
        main, extra = swapped_parts(chunk, main, extra)
        parts += [((chunk, True, True, True), extra), ((chunk, True, False, True), main)]
    result = place(shape, None, parts[:-1])
    result = place(shape, result, parts[-1:])
    return (squared, result)


def solution(mesh):
    return jax.shard_map(
        local,
        mesh=mesh,
        in_specs=(P("rows", None, None, None), P("rows", None, None, None), P(), P()),
        out_specs=(P("rows", None, None, None), P("rows", None, None, None)),
        check_vma=False,
    )
```

```python
import functools

import jax
import jax.numpy as jnp
from jax import lax
from jax.experimental import pallas as pl
from jax.experimental.pallas import tpu as pltpu
from jax.sharding import PartitionSpec as P


HALF = 2
KP = 2
CLASSES = 2 * HALF

COST = 2**20
VMEM_LIMIT = 16 * 2**20


def down_offset(panel, kind):
    return (kind - panel + HALF) % CLASSES - HALF


def classes_of(rep):
    return (rep % 2, rep % 2 + 2)


def route(panels, reps, target, kept=lambda panel, rep: True):
    pairs = []
    for rep in range(reps):
        for panel in range(panels):
            to_panel, to_rep = target(panel, rep)
            to_panel %= panels
            if kept(to_panel, to_rep):
                pairs.append((panel * reps + rep, to_panel * reps + to_rep))
    return pairs


def permute(block, pairs):
    return lax.ppermute(block, ("rows", "rep"), pairs)


def table_kernel(columns, table, *, blocks):
    count = columns.shape[0]
    device = lax.axis_index("rows")

    def one_row(i, carry):
        mine = [columns[u, device * blocks + i] for u in range(count)]
        for s in range(count):
            theirs = [columns[t, mine[s]] for t in range(count)]
            place = lax.rem(mine[s], blocks) * KP
            for u in range(count):
                offset = u // KP - s // KP
                found = jnp.int32(-1)
                if abs(offset) <= HALF:
                    for e in range(KP):
                        same = theirs[(offset + HALF) * KP + e] == mine[u]
                        found = jnp.where(same, place + e, found)
                table[(i * count + s) * count + u] = found
        return carry

    lax.fori_loop(0, blocks, one_row, 0)


def here(chunk, swapped=False):
    device, rep = lax.axis_index("rows"), lax.axis_index("rep")
    parity = lax.rem(rep + 1 if swapped else rep, 2)
    return down_offset(device, parity + 2 * chunk), lax.rem(device, 2) == 0


def row_product(left, regions, table, i, slot, begin, end):
    count = left.shape[1]

    def met(s, e):
        where = table[(i * count + s) * count + slot + e]
        tile = regions[s // KP][jnp.maximum(where, 0)]
        return jnp.where(where >= 0, tile, jnp.zeros_like(tile))

    lefts = jnp.concatenate([left[i, s] for s in range(begin, end)], axis=1)
    rights = jnp.concatenate(
        [jnp.concatenate([met(s, e) for e in range(KP)], axis=1) for s in range(begin, end)], axis=0
    )
    return jnp.dot(lefts, rights, preferred_element_type=jnp.float32)


def regions_of(parity, offset, own0, own1, core, near, two, forwarded):
    own = own0 if (offset == HALF) == (parity == 0) else own1
    if parity == 0:
        return (two, near, own, core, forwarded)
    return (forwarded, core, own, near, two)


def bounds_of(offset):
    return max(0, offset) * KP, (2 * HALF + 1 + min(0, offset)) * KP


def branches(chunk, run):
    mine, even = here(chunk)
    for parity in range(2):
        for offset in range(-HALF, HALF):

            @pl.when(jnp.logical_and(mine == offset, even == (parity == 0)))
            def _(parity=parity, offset=offset):
                run(parity, offset)


def halves(total):
    rounded = total.astype(jnp.bfloat16)
    tile = total.shape[0]
    return [rounded[:, e * tile : (e + 1) * tile] for e in range(KP)]


def first_kernel(chunk, table, coeffs, left, *refs):
    sources, (main, extra, send0, send1) = refs[:6], refs[6:]
    blocks, tile = left.shape[0], left.shape[2]

    def one_unit(parity, offset, sums, sends):
        slot = (offset + HALF) * KP
        regions = regions_of(parity, offset, *sources)

        def one_row(i, carry):
            total = row_product(left, regions, table, i, slot, *bounds_of(offset))
            for e, part in enumerate(halves(total)):
                sums[i, e] = part
                mixed = coeffs[1] * left[i, slot + e].astype(jnp.float32) + coeffs[2] * part.astype(
                    jnp.float32
                )
                if slot + e == HALF * KP:
                    line = lax.broadcasted_iota(jnp.int32, (tile, tile), 0)
                    column = lax.broadcasted_iota(jnp.int32, (tile, tile), 1)
                    mixed = jnp.where(line == column, coeffs[0], 0.0) + mixed
                for send in sends:
                    send[i, e] = mixed.astype(jnp.bfloat16)
            return carry

        lax.fori_loop(0, blocks, one_row, 0)

    def run(parity, offset):
        if offset > -HALF:
            one_unit(parity, offset, main, (send0, send1))
        else:
            one_unit(parity, -HALF, main, (send1 if parity == 0 else send0,))
            one_unit(parity, HALF, extra, (send0 if parity == 0 else send1,))

    branches(chunk, run)


def whole_kernel(chunk, table, left, own0, own1, core, forwarded, extra):
    def run(parity, offset):
        if offset > -HALF:
            return
        offset = HALF if parity == 0 else -HALF
        regions = regions_of(parity, offset, own0, own1, core, None, None, forwarded)

        def one_row(i, carry):
            total = row_product(
                left, regions, table, i, (offset + HALF) * KP, *bounds_of(offset)
            )
            for e, part in enumerate(halves(total)):
                extra[i, e] = part
            return carry

        lax.fori_loop(0, left.shape[0], one_row, 0)

    branches(chunk, run)


def part_kernel(chunk, table, left, own0, own1, core, near, forwarded, partial):
    count = left.shape[1]

    def run(parity, offset):
        if offset == -HALF and parity == 1:
            offset = HALF
        regions = regions_of(parity, offset, own0, own1, core, near, None, forwarded)
        begin, end = bounds_of(offset)
        begin, end = (max(begin, KP), end) if parity == 0 else (begin, min(end, count - KP))

        def one_row(i, carry):
            partial[i] = row_product(
                left, regions, table, i, (offset + HALF) * KP, begin, end
            )
            return carry

        lax.fori_loop(0, left.shape[0], one_row, 0)

    branches(chunk, run)


def late_kernel(chunk, table, left, two, partial, main):
    blocks, count = left.shape[0], left.shape[1]
    offset, even = here(chunk)
    odd = jnp.logical_not(even)
    slot = jnp.where(jnp.logical_and(offset == -HALF, odd), 2 * HALF, offset + HALF) * KP

    def rows(begin):
        def one_row(i, carry):
            total = partial[i] + row_product(
                left, (two,) * count, table, i, slot, begin, begin + KP
            )
            for e, part in enumerate(halves(total)):
                main[i, e] = part
            return carry

        lax.fori_loop(0, blocks, one_row, 0)

    pl.when(odd)(lambda: rows(count - KP))
    pl.when(jnp.logical_not(odd))(lambda: rows(0))


def call(kernel, operands, outs, scratch=(), full_at=None):
    arrays, specs = [], []
    for space, array in operands:
        specs.append(pl.BlockSpec(memory_space=space))
        if space in (pltpu.VMEM, pltpu.HBM):
            array = pltpu.with_memory_space_constraint(array, space)
        arrays.append(array)
    return pl.pallas_call(
        kernel,
        out_shape=[space(out.shape, out.dtype) for space, out in outs],
        in_specs=specs,
        out_specs=[pl.BlockSpec(memory_space=space) for space, _ in outs],
        scratch_shapes=scratch,
        input_output_aliases={} if full_at is None else {full_at: 0},
        compiler_params=pltpu.CompilerParams(vmem_limit_bytes=VMEM_LIMIT),
        cost_estimate=pl.CostEstimate(flops=COST, bytes_accessed=2**23, transcendentals=0),
    )(*arrays)


def units_of(tiles):
    blocks, tile = tiles.shape[0], tiles.shape[2]
    return pltpu.VMEM, jax.ShapeDtypeStruct((blocks, KP, tile, tile), tiles.dtype)


def flat(block):
    return pltpu.VMEM, block.reshape((-1,) + block.shape[2:])


def first_product(chunk, table, coeffs, left, rights):
    operands = [(pltpu.SMEM, table), (pltpu.SMEM, coeffs), (pltpu.VMEM, left)]
    return call(
        functools.partial(first_kernel, chunk),
        operands + [flat(r) for r in rights],
        [units_of(left)] * 4,
    )


def whole_product(chunk, table, left, rights):
    return call(
        functools.partial(whole_kernel, chunk),
        [(pltpu.SMEM, table), (pltpu.VMEM, left)] + [flat(rights[k]) for k in (0, 1, 2, 5)],
        [units_of(left)],
    )[0]


def part_product(chunk, table, left, rights):
    blocks, tile = left.shape[0], left.shape[2]
    partial = jax.ShapeDtypeStruct((blocks, tile, KP * tile), jnp.float32)
    return call(
        functools.partial(part_kernel, chunk),
        [(pltpu.SMEM, table), (pltpu.VMEM, left)] + [flat(rights[k]) for k in (0, 1, 2, 3, 5)],
        [(pltpu.VMEM, partial)],
    )[0]


def late_product(chunk, table, left, two, partial):
    return call(
        functools.partial(late_kernel, chunk),
        [(pltpu.SMEM, table), (pltpu.VMEM, left), flat(two), (pltpu.VMEM, partial)],
        [units_of(left)],
    )[0]


def place_kernel(names, aliased, *refs):
    parts, full, sems = refs[aliased : aliased + len(names)], refs[-2], refs[-1]
    slots, counts = [], []
    for chunk, swapped, second, mirrored in names:
        offset, even = here(chunk, swapped)
        both = offset == -HALF
        low = (offset + HALF) * KP
        high = 2 * HALF * KP
        turned = jnp.logical_and(both, jnp.logical_not(even))
        if second:
            slots.append(jnp.where(even, high, 0) if mirrored else high)
            counts.append(both)
        else:
            slots.append(jnp.where(turned, high, low) if mirrored else low)
            counts.append(None)

    def store(k):
        target = full.at[:, pl.ds(slots[k], KP)]
        return pltpu.make_async_copy(parts[k], target, sems.at[k])

    for step in (lambda k: store(k).start(), lambda k: store(k).wait()):
        for k, count in enumerate(counts):
            if count is None:
                step(k)
            else:
                pl.when(count)(functools.partial(step, k))


def place(shape, full, parts):
    names = tuple(name for name, _ in parts)
    units = [(pltpu.VMEM, unit) for _, unit in parts]
    aliased = 0 if full is None else 1
    return call(
        functools.partial(place_kernel, names, aliased),
        [(pltpu.HBM, full)] * aliased + units,
        [(pltpu.HBM, shape)],
        [pltpu.SemaphoreType.DMA((len(parts),))],
        0 if aliased else None,
    )[0]


def pick_kernel(chunk, tiles, out0, out1, sems):
    down, even = here(chunk)
    up = jnp.where(down == -HALF, HALF, down)
    offsets = (jnp.where(even, up, down), jnp.where(even, down, up))
    loads = [
        pltpu.make_async_copy(tiles.at[:, pl.ds((offsets[k] + HALF) * KP, KP)], out, sems.at[k])
        for k, out in enumerate((out0, out1))
    ]
    for load in loads:
        load.start()
    for load in loads:
        load.wait()


def pick(chunk, tiles):
    return call(
        functools.partial(pick_kernel, chunk),
        [(pltpu.HBM, tiles)],
        [units_of(tiles)] * 2,
        [pltpu.SemaphoreType.DMA((2,))],
    )


def tile_table(pattern, blocks):
    size = blocks * pattern.shape[1] ** 2
    return call(
        functools.partial(table_kernel, blocks=blocks),
        [(pltpu.SMEM, pattern.T)],
        [(pltpu.SMEM, jax.ShapeDtypeStruct((size,), jnp.int32))],
    )[0]


def local(x_tiles, giant_tiles, coeffs, pattern):
    blocks = x_tiles.shape[0]
    panels = lax.axis_size("rows")
    reps = lax.axis_size("rep")

    def swapped(panel):
        return panel + 1 if panel % 2 == 0 else panel - 1

    core_route = route(panels, reps, lambda p, z: (swapped(p), z))
    near_route = route(panels, reps, lambda p, z: (p - 1 if p % 2 == 0 else p + 1, z))

    def two_route(chunk):
        return route(
            panels,
            reps,
            lambda p, z: (p + 2 if p % 2 == 0 else p - 2, z),
            lambda p, z: (classes_of(z)[chunk] - p) % CLASSES != (1 if p % 2 == 0 else 3),
        )

    partner_route = route(panels, reps, lambda p, z: (p, z ^ 1))

    def extra_route(chunk):
        return route(
            panels,
            reps,
            lambda p, z: (p, z ^ 1),
            lambda p, z: down_offset(p, classes_of(z ^ 1)[chunk]) == -HALF,
        )

    def gathered(chunk, send0, send1):
        near = permute(send1, near_route)
        two = permute(send0, two_route(chunk))
        core = permute(send0, core_route)
        forwarded = permute(near, core_route)
        return (send0, send1, core, near, two, forwarded)

    def swapped_parts(chunk, main, extra):
        main = permute(main, partner_route)
        extra = permute(extra, extra_route(chunk))
        return main, extra

    rights = []
    for chunk in range(2):
        send0, send1 = pick(chunk, x_tiles)
        rights.append(gathered(chunk, send0, send1))
    table = tile_table(pattern, blocks)
    shape = jax.ShapeDtypeStruct(x_tiles.shape, x_tiles.dtype)

    babies = []
    parts = []
    for chunk in range(2):
        main, extra, send0, send1 = first_product(
            chunk, table, coeffs, x_tiles, rights[chunk]
        )
        babies.append(gathered(chunk, send0, send1))
        parts += [((chunk, False, False, False), main), ((chunk, False, True, False), extra)]
        main, extra = swapped_parts(chunk, main, extra)
        parts += [((chunk, True, False, False), main), ((chunk, True, True, False), extra)]
    squared = place(shape, None, parts)

    parts = []
    for chunk in range(2):
        extra = whole_product(chunk, table, giant_tiles, babies[chunk])
        partial = part_product(chunk, table, giant_tiles, babies[chunk])
        main = late_product(chunk, table, giant_tiles, babies[chunk][4], partial)
        parts += [((chunk, False, True, True), extra), ((chunk, False, False, True), main)]
        main, extra = swapped_parts(chunk, main, extra)
        parts += [((chunk, True, True, True), extra), ((chunk, True, False, True), main)]
    result = place(shape, None, parts[:-1])
    result = place(shape, result, parts[-1:])
    return (squared, result)


def solution(mesh):
    return jax.shard_map(
        local,
        mesh=mesh,
        in_specs=(P("rows", None, None, None), P("rows", None, None, None), P(), P()),
        out_specs=(P("rows", None, None, None), P("rows", None, None, None)),
        check_vma=False,
    )
```
